32 devices in a mesh: runs: 2 (over y), gx: 4 (over z), gy: 2 (over x), gz: 2 (over core).
Axes of the slice: x: 2, y: 2, z: 4, core: 2. Of those that a mesh axis runs over, the one named last changes fastest.
Arguments:
- positions: float32 [3, 8, 4096], P(None, None, ('runs', 'gx', 'gy', 'gz')), parts along dimension 2, as said below
- velocities: float32 [3, 8, 4096], P(None, None, ('runs', 'gx', 'gy', 'gz')), parts along dimension 2, may hold values from -5 to 5
- send_list: int32 [5696], P(('runs', 'gx', 'gy', 'gz')), parts along dimension 0, may hold values from 0 to 127, as said below
- pair_list: int32 [2, 57344], P(None, ('runs', 'gx', 'gy', 'gz')), parts along dimension 1, may hold values from 0 to 306, as said below
- constraint_flags: int32 [7, 4096], P(None, ('runs', 'gx', 'gy', 'gz')), parts along dimension 1, may hold values 0 or 1
Outputs:
- final_positions: float32 [3, 8, 4096], P(None, None, ('runs', 'gx', 'gy', 'gz')), parts along dimension 2
- final_velocities: float32 [3, 8, 4096], P(None, None, ('runs', 'gx', 'gy', 'gz')), parts along dimension 2
- energies: float32 [6, 2], P('runs'), parts along dimension 0
The draws below stay inside these ranges and needn't reach their ends.
There are 2 independent parts, one for each index of `runs`. The reference program is written for one: setup_inputs(seed, part) draws one part's arguments, and reference() takes and returns one part's arrays. A program takes and returns all parts, laid end to end along the dimension named above; each array names one. Nothing has to cross between parts.
Inputs may be any that keep to these rules, and one draw needn't show every extreme that they name: `send_list`: each domain's 178 entries are its own clusters (0 to 127, counted within the domain), in seven zone blocks of the sizes and order given in the reference program; a cluster may appear in several blocks. `pair_list`: each domain's 1792 slots name clusters of its extended set: 0 to 127 its own, then its received zone blocks in order; padding slots hold 306 in both rows; every cluster appears in a slot with itself; no unordered pair appears twice. `positions`: eight beads of a cluster lie in its cell of side 1, the cells of a domain filling a box of 1 by 8 by 16; neighbouring beads of a cluster are between 0.25 and 0.6 apart.
All inputs are finite; a program needn't handle non-finite values. No bound on the sum of `constraint_flags` on one device may be relied on, other than what follows from the above.
Results may differ from the reference program's by a relative error of at most 0.0003.
Values sent between devices are 32-bit elements; how exact they have to be, the bound alone decides.
A program may use at most 64 MiB of HBM per device.

```python
import jax
import jax.numpy as jnp
import numpy as np
from jax import lax

CX = 1
CY = 8
CZ = 16
ITERS = 3
NORDER = 4
NITER = 1
CL = 128
HC = 178
NP = 1792
DOMAINS = 16
NCL = 2048
BEADS = 16384
N_GX = 4
N_GY = 2
N_GZ = 2


zone_list = ((1, 0, 0), (0, 1, 0), (0, 0, 1), (1, 1, 0), (1, 0, 1), (0, 1, 1), (1, 1, 1))


def cluster_layout(key):
    layout_key = jax.random.fold_in(key, 101)
    scores = jax.random.randint(layout_key, (DOMAINS, CL), 0, 16384) * CL + jnp.arange(CL, dtype=jnp.int32)[None]
    cell_of_slot = jnp.argsort(scores, axis=1).astype(jnp.int32)
    slot_of_cell = jnp.argsort(cell_of_slot, axis=1).astype(jnp.int32)
    return (cell_of_slot, slot_of_cell)


def zone_cells(direction):
    cell_list = []
    for coord_x in [0] if direction[0] else range(CX):
        for coord_y in [0] if direction[1] else range(CY):
            for coord_z in [0] if direction[2] else range(CZ):
                cell_list.append((coord_x, coord_y, coord_z))
    return cell_list


def send_cells():
    linear = []
    for direction in zone_list:
        for cell in zone_cells(direction):
            linear.append((cell[0] * CY + cell[1]) * CZ + cell[2])
    return np.array(linear, np.int32)


def candidate_pairs():
    home_table = np.full((CX + 1, CY + 1, CZ + 1), -1, np.int32)
    halo_table = np.full((CX + 1, CY + 1, CZ + 1), -1, np.int32)
    for coord_x in range(CX):
        for coord_y in range(CY):
            for coord_z in range(CZ):
                home_table[coord_x, coord_y, coord_z] = (coord_x * CY + coord_y) * CZ + coord_z
    counter = CX * CY * CZ
    for direction in zone_list:
        for cell in zone_cells(direction):
            halo_table[cell[0] + direction[0] * CX, cell[1] + direction[1] * CY, cell[2] + direction[2] * CZ] = counter
            counter += 1
    dim_options = ((0, 0), (0, 1), (1, 0))
    patterns = []
    for first_dim in dim_options:
        for second_dim in dim_options:
            for third_dim in dim_options:
                pattern = (first_dim, second_dim, third_dim)
                leading = [entry for entry in pattern if entry != (0, 0)]
                if not leading or leading[0] == (0, 1):
                    patterns.append(pattern)
    first_home, first_halo, second_home, second_halo = ([], [], [], [])
    for coord_x in range(CX):
        for coord_y in range(CY):
            for coord_z in range(CZ):
                for pattern in patterns:
                    first_cell = (coord_x + pattern[0][0], coord_y + pattern[1][0], coord_z + pattern[2][0])
                    second_cell = (coord_x + pattern[0][1], coord_y + pattern[1][1], coord_z + pattern[2][1])
                    first_home.append(home_table[first_cell])
                    first_halo.append(halo_table[first_cell])
                    second_home.append(home_table[second_cell])
                    second_halo.append(halo_table[second_cell])
    return (np.array(first_home, np.int32), np.array(first_halo, np.int32), np.array(second_home, np.int32), np.array(second_halo, np.int32))


def draw_positions(key, part):
    cell_of_slot, slot_of_cell = cluster_layout(key)
    cell_x = cell_of_slot // (CY * CZ)
    cell_y = cell_of_slot // CZ % CY
    cell_z = cell_of_slot % CZ
    cell_coords = jnp.stack([cell_x, cell_y, cell_z]).astype(jnp.float32)
    beads = jnp.arange(8, dtype=jnp.float32)
    parity = (jnp.arange(8, dtype=jnp.int32) % 2).astype(jnp.float32)
    offsets = jnp.stack([0.115 + 0.11 * beads, 0.3 + 0.4 * parity, 0.115 + 0.11 * beads])
    spread = 0.03
    noise = jax.random.uniform(jax.random.fold_in(key, 202), (3, 8, DOMAINS, CL), jnp.float32, -spread, spread)
    result = cell_coords[:, None] + offsets[:, :, None, None] + noise
    return result.reshape(3, 8, DOMAINS * CL)


def draw_send_list(key, part):
    cell_of_slot, slot_of_cell = cluster_layout(key)
    return slot_of_cell[:, jnp.asarray(send_cells())].reshape(DOMAINS * HC).astype(jnp.int32)


def draw_pair_list(key, part):
    cell_of_slot, slot_of_cell = cluster_layout(key)
    first_home, first_halo, second_home, second_halo = candidate_pairs()
    padding = CL + HC

    def resolve(home_ids, halo_ids):
        from_home = slot_of_cell[:, jnp.asarray(np.maximum(home_ids, 0))]
        return jnp.where(jnp.asarray(home_ids >= 0)[None], from_home, jnp.asarray(halo_ids)[None])
    first_ids = resolve(first_home, first_halo)
    second_ids = resolve(second_home, second_halo)
    self_mask = jnp.asarray((first_home == second_home) & (first_halo == second_halo))[None]
    keep = (jax.random.randint(jax.random.fold_in(key, 303), (DOMAINS, NP), 0, 8) != 0) | self_mask
    first_ids = jnp.where(keep, first_ids, padding)
    second_ids = jnp.where(keep, second_ids, padding)
    order_scores = jax.random.randint(jax.random.fold_in(key, 404), (DOMAINS, NP), 0, 4096) * NP + jnp.arange(NP, dtype=jnp.int32)[None]
    shuffle = jnp.argsort(order_scores, axis=1)
    first_ids = jnp.take_along_axis(first_ids, shuffle, axis=1)
    second_ids = jnp.take_along_axis(second_ids, shuffle, axis=1)
    return jnp.stack([first_ids.reshape(-1), second_ids.reshape(-1)]).astype(jnp.int32)


def with_ends(values, key, smallest, high):
    place = [jax.random.randint(jax.random.fold_in(key, axis), (), 0, length) for axis, length in enumerate(values.shape)]
    longest = values.shape.index(max(values.shape))
    next_to = place[:longest] + [(place[longest] + 1) % values.shape[longest]] + place[longest + 1:]
    return values.at[tuple(place)].set(smallest).at[tuple(next_to)].set(high)


def level_of(stream_key, dims, cuts, least, top_value):
    def one(position, parts):
        heights = jax.random.uniform(jax.random.fold_in(jax.random.fold_in(stream_key, 6), position), (parts,), jnp.float32, least / len(cuts), top_value / len(cuts))
        return jnp.repeat(jnp.exp(heights), dims[position] // parts).reshape((-1,) + (1,) * (len(dims) - position - 1))

    factor_of = one(*cuts[0])
    for cut in cuts[1:]:
        factor_of = factor_of * one(*cut)
    return factor_of


def normal_values(stream_key, dims, scale, limit, shards=(), held_as=jnp.bfloat16):
    drawn = jax.random.normal(stream_key, dims, jnp.float32) * scale
    if len(shards) > 0:
        drawn = level_of(stream_key, dims, shards, -0.22, 0.18) * drawn
    return jnp.clip(drawn, min=-limit, max=limit).astype(held_as)


def setup_inputs(seed: int = 0, part: int = 0) -> dict:
    keys = jax.random.split(jax.random.key(seed), 6)
    own_keys = jax.random.split(jax.random.fold_in(keys[5], part), 6)
    positions = draw_positions(jax.random.fold_in(jax.random.fold_in(keys[5], part), 71), part)
    velocities = normal_values(own_keys[1], (3, 8, NCL), 1.0, 5.0, ((2, 16),), jnp.float32)
    send_list = draw_send_list(jax.random.fold_in(jax.random.fold_in(keys[5], part), 71), part)
    pair_list = draw_pair_list(jax.random.fold_in(jax.random.fold_in(keys[5], part), 71), part)
    constraint_flags = with_ends((jax.random.randint(own_keys[4], (7, NCL), 0, 4) < 3).astype(jnp.int32), jax.random.fold_in(own_keys[4], 1), 0, 1)
    return dict(positions=positions, velocities=velocities, send_list=send_list, pair_list=pair_list, constraint_flags=constraint_flags)


time_step = 0.02
strength = 2.0
root_half = 0.7071067811865476
zone_list = ((1, 0, 0), (0, 1, 0), (0, 0, 1), (1, 1, 0), (1, 0, 1), (0, 1, 1), (1, 1, 1))

def zone_sizes():
    return tuple(((CX if direction[0] == 0 else 1) * (CY if direction[1] == 0 else 1) * (CZ if direction[2] == 0 else 1) for direction in zone_list))

def zone_starts():
    block_sizes = zone_sizes()
    return tuple((sum(block_sizes[:number]) for number in range(7)))

def pair_kernel(extended, first_ids, second_ids):
    dummy_index = extended.shape[2] - 1
    first_coords = jnp.take(extended, first_ids, axis=2)
    second_coords = jnp.take(extended, second_ids, axis=2)
    separation = first_coords[:, :, None, :] - second_coords[:, None, :, :]
    scaled = lax.optimization_barrier(jnp.sum(separation * separation, axis=0))
    intersect = jnp.maximum(1.0 - scaled, 0.0)
    bead_row = lax.broadcasted_iota(jnp.int32, (8, 8, 1), 0)
    bead_column = lax.broadcasted_iota(jnp.int32, (8, 8, 1), 1)
    self_pair = (first_ids == second_ids)[None, None, :]
    usable = (first_ids < dummy_index)[None, None, :]
    weight = (jnp.where(self_pair, bead_row < bead_column, True) & usable).astype(jnp.float32)
    energy = strength * jnp.sum(weight * intersect * intersect * intersect)
    magnitude = 6.0 * strength * weight * intersect * intersect
    pushing = magnitude[None] * separation
    return (lax.optimization_barrier(jnp.sum(pushing, axis=2)), -lax.optimization_barrier(jnp.sum(pushing, axis=1)), energy)

def domain_forces(extended, pair_ids):
    first_blocks = pair_ids[0].reshape(28, -1)
    second_blocks = pair_ids[1].reshape(28, -1)

    def accumulate(state, blocks):
        forces, energy = state
        on_first, on_second, block_energy = pair_kernel(extended, blocks[0], blocks[1])
        forces = forces.at[:, :, blocks[0]].add(on_first)
        forces = forces.at[:, :, blocks[1]].add(on_second)
        return ((forces, energy + block_energy), None)
    initial = (jnp.zeros(extended.shape, jnp.float32), jnp.zeros((), jnp.float32))
    result = lax.scan(accumulate, initial, (first_blocks, second_blocks))
    return result[0]

def total_forces(coords, send_list, pair_list):
    grid_shape = (N_GX, N_GY, N_GZ)
    domain_count = N_GX * N_GY * N_GZ
    home_coords = coords.reshape((3, 8) + grid_shape + (CL,))
    send_grid = send_list.reshape(grid_shape + (HC,))
    block_sizes = zone_sizes()
    starts = zone_starts()
    pieces = []
    for number in range(7):
        direction = zone_list[number]
        backward = tuple((-component for component in direction))
        source = jnp.roll(home_coords, backward, axis=(2, 3, 4))
        chosen = jnp.roll(send_grid, backward, axis=(0, 1, 2))[..., starts[number]:starts[number] + block_sizes[number]]
        chosen = jnp.broadcast_to(chosen[None, None], (3, 8) + grid_shape + (block_sizes[number],))
        gathered = jnp.take_along_axis(source, chosen, axis=5)
        offset = jnp.array([direction[0] * CX, direction[1] * CY, direction[2] * CZ], jnp.float32)
        pieces.append(gathered + offset[:, None, None, None, None, None])
    dummy_cluster = jnp.zeros((3, 8) + grid_shape + (1,), jnp.float32)
    extended = jnp.concatenate([home_coords] + pieces + [dummy_cluster], axis=5)
    extended = jnp.moveaxis(extended.reshape(3, 8, domain_count, CL + HC + 1), 2, 0)
    domain_pairs = jnp.moveaxis(pair_list.reshape(2, domain_count, 14 * CL), 1, 0)
    forces, energies = lax.map(lambda pair_data: domain_forces(pair_data[0], pair_data[1]), (extended, domain_pairs))
    forces = jnp.moveaxis(forces, 0, 2)
    flat_home = forces[:, :, :, :CL].reshape(3, 8, domain_count * CL)
    halo_forces = forces[:, :, :, CL:CL + HC].reshape((3, 8) + grid_shape + (HC,))
    domain_base = (jnp.arange(domain_count, dtype=jnp.int32) * CL).reshape(grid_shape + (1,))
    for number in range(7):
        direction = zone_list[number]
        zone_forces = halo_forces[..., starts[number]:starts[number] + block_sizes[number]]
        zone_forces = jnp.roll(zone_forces, direction, axis=(2, 3, 4))
        targets = (send_grid[..., starts[number]:starts[number] + block_sizes[number]] + domain_base).reshape(-1)
        flat_home = flat_home.at[:, :, targets].add(zone_forces.reshape(3, 8, -1))
    return (flat_home, jnp.sum(energies))

def link_vectors(coords):
    return coords[:, :-1, :] - coords[:, 1:, :]

def link_lengths(coords):
    vectors = link_vectors(coords)
    return jnp.sqrt(lax.optimization_barrier(jnp.sum(vectors * vectors, axis=0)))

def expand(coupling, source):
    coupling_down = jnp.pad(coupling, ((1, 0), (0, 0)))
    coupling_up = jnp.pad(coupling, ((0, 1), (0, 0)))
    series = source
    result = source
    for expansion in range(NORDER):
        series = coupling_down * jnp.pad(series, ((1, 0), (0, 0)))[:-1] + coupling_up * jnp.pad(series, ((0, 1), (0, 0)))[1:]
        result = result + series
    return result

def apply_links(coords, directions, solution):
    shifts = directions * (root_half * solution)[None]
    return coords - jnp.pad(shifts, ((0, 0), (0, 1), (0, 0))) + jnp.pad(shifts, ((0, 0), (1, 0), (0, 0)))

def constrain(previous, updated, rest_length, link_flags):
    old_vectors = link_vectors(previous)
    directions = old_vectors / jnp.maximum(jnp.sqrt(lax.optimization_barrier(jnp.sum(old_vectors * old_vectors, axis=0))), 0.2)[None]
    coupling = 0.5 * lax.optimization_barrier(jnp.sum(directions[:, :-1] * directions[:, 1:], axis=0)) * link_flags[:-1] * link_flags[1:]
    projected = lax.optimization_barrier(jnp.sum(directions * link_vectors(updated), axis=0))
    solution = expand(coupling, link_flags * root_half * (projected - rest_length))
    updated = apply_links(updated, directions, solution)
    for correction in range(NITER):
        vectors = link_vectors(updated)
        squared = lax.optimization_barrier(jnp.sum(vectors * vectors, axis=0))
        target = jnp.sqrt(jnp.maximum(2.0 * rest_length * rest_length - squared, 0.25 * rest_length * rest_length))
        solution = expand(coupling, link_flags * root_half * (rest_length - target))
        updated = apply_links(updated, directions, solution)
    return updated

def reference(positions, velocities, send_list, pair_list, constraint_flags):
    link_flags = constraint_flags.astype(jnp.float32)
    rest_length = link_lengths(positions)
    forces, potential = total_forces(positions, send_list, pair_list)
    energy_rows = []
    for iteration in range(ITERS):
        half_speed = velocities + 0.5 * time_step * forces
        updated = constrain(positions, positions + time_step * half_speed, rest_length, link_flags)
        half_speed = (updated - positions) / time_step
        forces, potential = total_forces(updated, send_list, pair_list)
        velocities = half_speed + 0.5 * time_step * forces
        positions = updated
        kinetic = 0.5 * jnp.sum(velocities * velocities)
        energy_rows.append(jnp.stack([potential, kinetic]))
    energies = jnp.stack(energy_rows) / BEADS
    return (positions, velocities, energies)
```

```python
import functools
import itertools

import jax
import jax.numpy as jnp
from jax import lax
from jax.experimental import pallas as pl
from jax.experimental.pallas import tpu as pltpu
from jax.sharding import PartitionSpec as P

CX = 1
CY = 8
CZ = 16
ITERS = 3
NORDER = 4
NITER = 1

MESH = pl.DeviceIdType.MESH
AXES = ("gx", "gy", "gz")
LANES = 128

time_step = 0.02
strength = 2.0
root_half = 0.7071067811865476
zone_list = ((1, 0, 0), (0, 1, 0), (0, 0, 1), (1, 1, 0), (1, 0, 1), (0, 1, 1), (1, 1, 1))


def zone_sizes():
    return tuple(
        (CX if d[0] == 0 else 1) * (CY if d[1] == 0 else 1) * (CZ if d[2] == 0 else 1)
        for d in zone_list
    )


def zone_spans():
    spans = []
    position = 0
    for size in zone_sizes()[1:]:
        spans.append((position, position + size))
        position += size
    return spans


def neighbour(sizes, direction, sign):
    ids = {}
    for axis, size, step in zip(AXES, sizes, direction):
        if step:
            ids[axis] = lax.rem(lax.axis_index(axis) + (size + sign * step), size)
    return ids


def peer(sizes, number):
    _, ny, nz = sizes
    steps = (number // (ny * nz), (number // nz) % ny, number % nz)
    return {
        axis: lax.rem(lax.axis_index(axis) + step, size)
        for axis, size, step in zip(AXES, sizes, steps)
    }


def each_peer(sizes, body):
    count = sizes[0] * sizes[1] * sizes[2]
    if count <= 32:
        for number in range(1, count):
            body(number)
    else:

        def step(number, carry):
            body(number)
            return carry

        lax.fori_loop(1, count, step, 0)


def up(value):
    return pltpu.roll(value, 7, 0)


def down(value):
    return pltpu.roll(value, 1, 0)


def dot3(a, b):
    return a[0] * b[0] + a[1] * b[1] + a[2] * b[2]


def expand(coupling, source):
    coupling_down = down(coupling)
    series = source
    result = source
    for _ in range(NORDER):
        series = coupling_down * down(series) + coupling * up(series)
        result = result + series
    return result


def apply_links(coords, directions, solution):
    scaled = root_half * solution
    moved = []
    for c in range(3):
        shift = directions[c] * scaled
        moved.append(coords[c] - shift + down(shift))
    return moved


def take_lanes(value, lanes):
    return jnp.take_along_axis(value, lanes, axis=1, mode="promise_in_bounds")


def merge_zones(parts, fill):
    lane = lax.broadcasted_iota(jnp.int32, (8, LANES), 1)
    spans = zone_spans()
    merged = fill
    for number in reversed(range(6)):
        low, high = spans[number]
        merged = jnp.where((lane >= low) & (lane < high), parts[number], merged)
    return merged


def halo_offset(c):
    lane = lax.broadcasted_iota(jnp.int32, (8, LANES), 1)
    offset = jnp.zeros((8, LANES), jnp.float32)
    for number, (low, high) in enumerate(zone_spans()):
        if zone_list[number + 1][c]:
            offset = jnp.where(
                (lane >= low) & (lane < high), float((CX, CY, CZ)[c]), offset
            )
    return offset


def kernel(
    sizes,
    unroll,
    pos_ref,
    vel_ref,
    send_ref,
    pair_ref,
    flag_ref,
    out_x,
    out_v,
    out_e,
    table,
    home,
    weights,
    ext,
    zin,
    cout,
    fout,
    fin,
    fbuf,
    force,
    unit,
    couple,
    eacc,
    eout,
    ein,
    send_sem,
    recv_sem,
    fsend_sem,
    frecv_sem,
    esend_sem,
    erecv_sem,
):
    slots = pair_ref.shape[1]
    tiles = slots // LANES
    bead = lax.broadcasted_iota(jnp.int32, (8, LANES), 0)
    count = sizes[0] * sizes[1] * sizes[2]
    pad_index = 2 * LANES + zone_spans()[-1][1]

    barrier = pltpu.get_barrier_semaphore()

    def greet(number):
        pl.semaphore_signal(barrier, inc=1, device_id=peer(sizes, number), device_id_type=MESH)

    each_peer(sizes, greet)

    out_x[...] = pos_ref[...]
    out_v[...] = vel_ref[...]
    flags = jnp.concatenate(
        [flag_ref[...].astype(jnp.float32), jnp.zeros((1, LANES), jnp.float32)], axis=0
    )
    flags_up = up(flags)
    first = [pos_ref[c] for c in range(3)]
    links = [a - up(a) for a in first]
    rest = jnp.sqrt(dot3(links, links))

    pl.semaphore_wait(barrier, count - 1)

    def coord_copy(zone):
        return pltpu.make_async_remote_copy(
            src_ref=cout.at[0 if zone == 0 else 1],
            dst_ref=zin.at[zone],
            send_sem=send_sem.at[zone],
            recv_sem=recv_sem.at[zone],
            device_id=neighbour(sizes, zone_list[zone], -1),
            device_id_type=MESH,
        )

    def force_copy(zone):
        return pltpu.make_async_remote_copy(
            src_ref=fout.at[0 if zone == 0 else 1],
            dst_ref=fin.at[zone],
            send_sem=fsend_sem.at[zone],
            recv_sem=frecv_sem.at[zone],
            device_id=neighbour(sizes, zone_list[zone], 1),
            device_id_type=MESH,
        )

    order = (6, 3, 4, 0, 1, 5, 2)

    def evaluate():
        for half in (1, 0):
            lanes = jnp.broadcast_to(send_ref[half : half + 1, :], (8, LANES))
            for c in range(3):
                cout[half, c] = take_lanes(out_x[c], lanes)
        copies = [coord_copy(zone) for zone in range(7)]
        for zone in order:
            copies[zone].start()

    def prepare():
        old = [out_x[c] for c in range(3)]
        vectors = [a - up(a) for a in old]
        length = jnp.maximum(jnp.sqrt(dot3(vectors, vectors)), 0.2)
        directions = [a / length for a in vectors]
        for c in range(3):
            unit[c] = directions[c]
        couple[...] = 0.5 * dot3(directions, [up(a) for a in directions]) * flags * flags_up

    def build_tables():
        lane = lax.broadcasted_iota(jnp.int32, (LANES, LANES), 1)
        for half in range(2):
            rows = jnp.broadcast_to(send_ref[half : half + 1, :], (LANES, LANES)).T
            home[half * LANES : (half + 1) * LANES, :] = (
                (rows == lane).astype(jnp.float32).astype(jnp.bfloat16)
            )

        def build(tile, carry):
            at = pl.ds(pl.multiple_of(tile * LANES, LANES), LANES)
            for side in range(2):
                rows = jnp.broadcast_to(pair_ref[side : side + 1, at], (LANES, LANES)).T
                start = pl.multiple_of(side * slots + tile * LANES, LANES)
                for block in range(3):
                    table[pl.ds(start, LANES), block * LANES : (block + 1) * LANES] = (
                        (rows == lane + block * LANES).astype(jnp.float32).astype(jnp.bfloat16)
                    )
            one = jnp.broadcast_to(pair_ref[0:1, at], (8, LANES))
            two = jnp.broadcast_to(pair_ref[1:2, at], (8, LANES))
            for shift in range(8):
                use = one != two
                if shift:
                    use = use | (bead < 8 - shift)
                use = use & (one != pad_index)
                weights[tile, shift] = use.astype(jnp.float32)
            return carry

        lax.fori_loop(0, tiles, build, 0)

    def receive_coords():
        for c in range(3):
            ext[0, c] = out_x[c]
        copies = [coord_copy(zone) for zone in range(7)]
        for zone in range(7):
            copies[zone].wait()
        for c in range(3):
            ext[1, c] = zin[0, c] + float(CX if c == 0 else 0)
            merged = merge_zones(
                [zin[zone, c] for zone in range(1, 7)], jnp.zeros((8, LANES), jnp.float32)
            )
            ext[2, c] = merged + halo_offset(c)

    def pairs():
        def tile_step(tile, energy):
            at = pl.ds(pl.multiple_of(tile * LANES, LANES), LANES)
            beads = []
            for side in range(2):
                index = jnp.broadcast_to(pair_ref[side : side + 1, at], (8, LANES))
                lanes = index & (LANES - 1)
                in_own = index < LANES
                in_first = index < 2 * LANES
                beads.append(
                    [
                        jnp.where(
                            in_own,
                            take_lanes(ext[0, c], lanes),
                            jnp.where(
                                in_first,
                                take_lanes(ext[1, c], lanes),
                                take_lanes(ext[2, c], lanes),
                            ),
                        )
                        for c in range(3)
                    ]
                )
            on_first = [None] * 3
            on_second = [None] * 3
            for shift in range(8):
                gap = []
                for c in range(3):
                    other = beads[1][c]
                    if shift:
                        other = pltpu.roll(other, 8 - shift, 0)
                    gap.append(beads[0][c] - other)
                reach = jnp.maximum(weights[tile, shift] - dot3(gap, gap), 0.0)
                square = reach * reach
                energy = energy + square * reach
                for c in range(3):
                    push = square * gap[c]
                    back = pltpu.roll(push, shift, 0) if shift else push
                    on_first[c] = push if shift == 0 else on_first[c] + push
                    on_second[c] = -back if shift == 0 else on_second[c] - back
            for side, parts in enumerate((on_first, on_second)):
                start = pl.multiple_of(side * slots + tile * LANES, LANES)
                for c in range(3):
                    high = parts[c].astype(jnp.bfloat16).astype(jnp.float32)
                    fbuf[c * 8 : c * 8 + 8, pl.ds(start, LANES)] = high
                    fbuf[24 + c * 8 : 32 + c * 8, pl.ds(start, LANES)] = parts[c] - high
            return energy

        def group(number, energy):
            for inner in range(unroll):
                energy = tile_step(number * unroll + inner, energy)
            return energy

        return lax.fori_loop(0, tiles // unroll, group, jnp.zeros((8, LANES), jnp.float32))

    def scatter():
        values = fbuf[...].astype(jnp.bfloat16)
        halo = jnp.dot(values, table[:, LANES:], preferred_element_type=jnp.float32)
        halo = (6.0 * strength) * (halo[:24] + halo[24:])
        for half in (1, 0):
            for c in range(3):
                fout[half, c] = halo[c * 8 : c * 8 + 8, half * LANES : (half + 1) * LANES]
        copies = [force_copy(zone) for zone in range(7)]
        for zone in order:
            copies[zone].start()
        own = jnp.dot(values, table[:, :LANES], preferred_element_type=jnp.float32)
        own = (6.0 * strength) * (own[:24] + own[24:])
        for zone in range(7):
            copies[zone].wait()
        zero = jnp.zeros((8, LANES), jnp.float32)
        rows = []
        for c in range(3):
            merged = merge_zones([fin[zone, c] for zone in range(1, 7)], zero)
            rows.append(jnp.concatenate([fin[0, c], merged], axis=1))
        back = jnp.concatenate(rows, axis=0)
        high = back.astype(jnp.bfloat16).astype(jnp.float32)
        split = jnp.concatenate([high, back - high], axis=0).astype(jnp.bfloat16)
        added = jnp.dot(split, home[...], preferred_element_type=jnp.float32)
        total = own + added[:24] + added[24:]
        for c in range(3):
            force[c] = total[c * 8 : c * 8 + 8]

    def integrate():
        old = [out_x[c] for c in range(3)]
        half = [out_v[c] + (0.5 * time_step) * force[c] for c in range(3)]
        moved = [old[c] + time_step * half[c] for c in range(3)]
        directions = [unit[c] for c in range(3)]
        coupling = couple[...]
        vectors = [a - up(a) for a in moved]
        projected = dot3(directions, vectors)
        solved = expand(coupling, flags * root_half * (projected - rest))
        moved = apply_links(moved, directions, solved)
        for _ in range(NITER):
            vectors = [a - up(a) for a in moved]
            squared = dot3(vectors, vectors)
            target = jnp.sqrt(jnp.maximum(2.0 * rest * rest - squared, 0.25 * rest * rest))
            solved = expand(coupling, flags * root_half * (rest - target))
            moved = apply_links(moved, directions, solved)
        for c in range(3):
            out_v[c] = (moved[c] - old[c]) / time_step
            out_x[c] = moved[c]

    def step(number, carry):
        @pl.when(number > 0)
        def _():
            integrate()

        evaluate()
        prepare()

        @pl.when(number == 0)
        def _():
            build_tables()

        receive_coords()
        energy = pairs()
        scatter()

        @pl.when(number > 0)
        def _():
            speeds = [out_v[c] + (0.5 * time_step) * force[c] for c in range(3)]
            for c in range(3):
                out_v[c] = speeds[c]
            eacc[2 * (number - 1)] = strength * energy
            eacc[2 * (number - 1) + 1] = 0.5 * dot3(speeds, speeds)

        return carry

    lax.fori_loop(0, ITERS + 1, step, 0)

    total = jnp.zeros((8, LANES), jnp.float32)
    for row in range(2 * ITERS):
        line = jnp.sum(eacc[row], axis=0, keepdims=True)
        total = jnp.where(bead == row, line, total)
    eout[...] = total

    def energy_copy(number):
        return pltpu.make_async_remote_copy(
            src_ref=eout,
            dst_ref=ein.at[number],
            send_sem=esend_sem.at[number],
            recv_sem=erecv_sem.at[number],
            device_id=peer(sizes, number),
            device_id_type=MESH,
        )

    each_peer(sizes, lambda number: energy_copy(number).start())
    each_peer(sizes, lambda number: energy_copy(number).wait())
    if count <= 32:
        for number in range(1, count):
            total = total + ein[number]
    else:
        total = lax.fori_loop(1, count, lambda number, acc: acc + ein[number], total)
    beads = 8 * LANES * count
    summed = jnp.sum(total, axis=1, keepdims=True) / beads
    for row in range(ITERS):
        for column in range(2):
            at = 2 * row + column
            out_e[row : row + 1, column : column + 1] = summed[at : at + 1, :]


def on_device(sizes, positions, velocities, send_list, pair_list, constraint_flags):
    clusters = positions.shape[2]
    slots = pair_list.shape[1]
    tiles = slots // LANES
    count = sizes[0] * sizes[1] * sizes[2]
    unroll = max(u for u in range(1, 8) if tiles % u == 0)
    sends = jnp.pad(send_list, (0, 2 * LANES - send_list.shape[0])).reshape(2, LANES)
    vmem = pl.BlockSpec(memory_space=pltpu.VMEM)
    f32 = jnp.float32
    return pl.pallas_call(
        functools.partial(kernel, sizes, unroll),
        out_shape=(
            jax.ShapeDtypeStruct(positions.shape, f32),
            jax.ShapeDtypeStruct(velocities.shape, f32),
            jax.ShapeDtypeStruct((ITERS, 2), f32),
        ),
        in_specs=[vmem] * 5,
        out_specs=(vmem, vmem, vmem),
        scratch_shapes=[
            pltpu.VMEM((2 * slots, 3 * clusters), jnp.bfloat16),
            pltpu.VMEM((2 * clusters, clusters), jnp.bfloat16),
            pltpu.VMEM((tiles, 8, 8, LANES), f32),
            pltpu.VMEM((3, 3, 8, LANES), f32),
            pltpu.VMEM((7, 3, 8, LANES), f32),
            pltpu.VMEM((2, 3, 8, LANES), f32),
            pltpu.VMEM((2, 3, 8, LANES), f32),
            pltpu.VMEM((7, 3, 8, LANES), f32),
            pltpu.VMEM((48, 2 * slots), f32),
            pltpu.VMEM((3, 8, LANES), f32),
            pltpu.VMEM((3, 8, LANES), f32),
            pltpu.VMEM((8, LANES), f32),
            pltpu.VMEM((2 * ITERS, 8, LANES), f32),
            pltpu.VMEM((8, LANES), f32),
            pltpu.VMEM((count, 8, LANES), f32),
            pltpu.SemaphoreType.DMA((7,)),
            pltpu.SemaphoreType.DMA((7,)),
            pltpu.SemaphoreType.DMA((7,)),
            pltpu.SemaphoreType.DMA((7,)),
            pltpu.SemaphoreType.DMA((count,)),
            pltpu.SemaphoreType.DMA((count,)),
        ],
        compiler_params=pltpu.CompilerParams(collective_id=0, has_side_effects=True),
    )(positions, velocities, sends, pair_list, constraint_flags)


def solution(mesh):
    sizes = tuple(mesh.shape[axis] for axis in AXES)
    split = ("runs", "gx", "gy", "gz")
    return jax.shard_map(
        functools.partial(on_device, sizes),
        mesh=mesh,
        in_specs=(
            P(None, None, split),
            P(None, None, split),
            P(split),
            P(None, split),
            P(None, split),
        ),
        out_specs=(P(None, None, split), P(None, None, split), P("runs", None)),
        check_vma=False,
    )
```

```python
import functools
import itertools

import jax
import jax.numpy as jnp
from jax import lax
from jax.experimental import pallas as pl
from jax.experimental.pallas import tpu as pltpu
from jax.sharding import PartitionSpec as P

CX = 1
CY = 8
CZ = 16
ITERS = 3
NORDER = 4
NITER = 1

MESH = pl.DeviceIdType.MESH
AXES = ("gx", "gy", "gz")
LANES = 128

time_step = 0.02
strength = 2.0
root_half = 0.7071067811865476
zone_list = ((1, 0, 0), (0, 1, 0), (0, 0, 1), (1, 1, 0), (1, 0, 1), (0, 1, 1), (1, 1, 1))


def zone_sizes():
    return tuple(
        (CX if d[0] == 0 else 1) * (CY if d[1] == 0 else 1) * (CZ if d[2] == 0 else 1)
        for d in zone_list
    )


def zone_spans():
    spans = []
    position = 0
    for size in zone_sizes()[1:]:
        spans.append((position, position + size))
        position += size
    return spans


def neighbour(sizes, direction, sign):
    ids = {}
    for axis, size, step in zip(AXES, sizes, direction):
        if step:
            ids[axis] = lax.rem(lax.axis_index(axis) + (size + sign * step), size)
    return ids


def peer(sizes, number):
    _, ny, nz = sizes
    steps = (number // (ny * nz), (number // nz) % ny, number % nz)
    return {
        axis: lax.rem(lax.axis_index(axis) + step, size)
        for axis, size, step in zip(AXES, sizes, steps)
    }


def each_peer(sizes, body):
    count = sizes[0] * sizes[1] * sizes[2]
    if count <= 32:
        for number in range(1, count):
            body(number)
    else:

        def step(number, carry):
            body(number)
            return carry

        lax.fori_loop(1, count, step, 0)


def up(value):
    return pltpu.roll(value, 7, 0)


def down(value):
    return pltpu.roll(value, 1, 0)


def dot3(a, b):
    return a[0] * b[0] + a[1] * b[1] + a[2] * b[2]


def expand(coupling, source):
    coupling_down = down(coupling)
    series = source
    result = source
    for _ in range(NORDER):
        series = coupling_down * down(series) + coupling * up(series)
        result = result + series
    return result


def apply_links(coords, directions, solution):
    scaled = root_half * solution
    moved = []
    for c in range(3):
        shift = directions[c] * scaled
        moved.append(coords[c] - shift + down(shift))
    return moved


def take_lanes(value, lanes):
    return jnp.take_along_axis(value, lanes, axis=1, mode="promise_in_bounds")


def merge_zones(parts, fill):
    lane = lax.broadcasted_iota(jnp.int32, (8, LANES), 1)
    spans = zone_spans()
    merged = fill
    for number in reversed(range(6)):
        low, high = spans[number]
        merged = jnp.where((lane >= low) & (lane < high), parts[number], merged)
    return merged


def halo_offset(c):
    lane = lax.broadcasted_iota(jnp.int32, (8, LANES), 1)
    offset = jnp.zeros((8, LANES), jnp.float32)
    for number, (low, high) in enumerate(zone_spans()):
        if zone_list[number + 1][c]:
            offset = jnp.where(
                (lane >= low) & (lane < high), float((CX, CY, CZ)[c]), offset
            )
    return offset


def kernel(
    sizes,
    unroll,
    pos_hbm,
    vel_hbm,
    send_hbm,
    pair_hbm,
    flag_hbm,
    out_x,
    out_v,
    out_e,
    send_flat,
    send_ref,
    pair_ref,
    flag_ref,
    load_sem,
    table,
    home,
    weights,
    ext,
    zin,
    cout,
    fout,
    fin,
    fbuf,
    force,
    unit,
    couple,
    eacc,
    eout,
    ein,
    send_sem,
    recv_sem,
    fsend_sem,
    frecv_sem,
    esend_sem,
    erecv_sem,
):
    slots = pair_ref.shape[1]
    tiles = slots // LANES
    bead = lax.broadcasted_iota(jnp.int32, (8, LANES), 0)
    count = sizes[0] * sizes[1] * sizes[2]
    pad_index = 2 * LANES + zone_spans()[-1][1]

    barrier = pltpu.get_barrier_semaphore()

    def greet(number):
        pl.semaphore_signal(barrier, inc=1, device_id=peer(sizes, number), device_id_type=MESH)

    each_peer(sizes, greet)

    loads = [
        pltpu.make_async_copy(source, target, load_sem.at[number])
        for number, (source, target) in enumerate(
            (
                (pos_hbm, out_x),
                (send_hbm, send_flat),
                (pair_hbm, pair_ref),
                (flag_hbm, flag_ref),
                (vel_hbm, out_v),
            )
        )
    ]
    for load in loads:
        load.start()
    for load in loads:
        load.wait()
    small = send_flat.shape[0] - LANES
    send_ref[0:1, :] = send_flat[0:LANES].reshape(1, LANES)
    send_ref[1:2, :] = jnp.concatenate(
        [send_flat[LANES:], jnp.zeros((LANES - small,), jnp.int32)]
    ).reshape(1, LANES)
    flags = jnp.concatenate(
        [flag_ref[...].astype(jnp.float32), jnp.zeros((1, LANES), jnp.float32)], axis=0
    )
    flags_up = up(flags)
    first = [out_x[c] for c in range(3)]
    links = [a - up(a) for a in first]
    rest = jnp.sqrt(dot3(links, links))

    pl.semaphore_wait(barrier, count - 1)

    def coord_copy(zone):
        return pltpu.make_async_remote_copy(
            src_ref=cout.at[0 if zone == 0 else 1],
            dst_ref=zin.at[zone],
            send_sem=send_sem.at[zone],
            recv_sem=recv_sem.at[zone],
            device_id=neighbour(sizes, zone_list[zone], -1),
            device_id_type=MESH,
        )

    def force_copy(zone):
        return pltpu.make_async_remote_copy(
            src_ref=fout.at[0 if zone == 0 else 1],
            dst_ref=fin.at[zone],
            send_sem=fsend_sem.at[zone],
            recv_sem=frecv_sem.at[zone],
            device_id=neighbour(sizes, zone_list[zone], 1),
            device_id_type=MESH,
        )

    order = (6, 3, 4, 0, 1, 5, 2)

    def evaluate():
        for half in (1, 0):
            lanes = jnp.broadcast_to(send_ref[half : half + 1, :], (8, LANES))
            for c in range(3):
                cout[half, c] = take_lanes(out_x[c], lanes)
        copies = [coord_copy(zone) for zone in range(7)]
        for zone in order:
            copies[zone].start()

    def prepare():
        old = [out_x[c] for c in range(3)]
        vectors = [a - up(a) for a in old]
        length = jnp.maximum(jnp.sqrt(dot3(vectors, vectors)), 0.2)
        directions = [a / length for a in vectors]
        for c in range(3):
            unit[c] = directions[c]
        couple[...] = 0.5 * dot3(directions, [up(a) for a in directions]) * flags * flags_up

    def build_tables():
        lane = lax.broadcasted_iota(jnp.int32, (LANES, LANES), 1)
        for half in range(2):
            rows = jnp.broadcast_to(send_ref[half : half + 1, :], (LANES, LANES)).T
            home[half * LANES : (half + 1) * LANES, :] = (
                (rows == lane).astype(jnp.float32).astype(jnp.bfloat16)
            )

        def build(tile, carry):
            at = pl.ds(pl.multiple_of(tile * LANES, LANES), LANES)
            for side in range(2):
                rows = jnp.broadcast_to(pair_ref[side : side + 1, at], (LANES, LANES)).T
                start = pl.multiple_of(side * slots + tile * LANES, LANES)
                for block in range(3):
                    table[pl.ds(start, LANES), block * LANES : (block + 1) * LANES] = (
                        (rows == lane + block * LANES).astype(jnp.float32).astype(jnp.bfloat16)
                    )
            one = jnp.broadcast_to(pair_ref[0:1, at], (8, LANES))
            two = jnp.broadcast_to(pair_ref[1:2, at], (8, LANES))
            for shift in range(8):
                use = one != two
                if shift:
                    use = use | (bead < 8 - shift)
                use = use & (one != pad_index)
                weights[tile, shift] = use.astype(jnp.float32)
            return carry

        lax.fori_loop(0, tiles, build, 0)

    def receive_coords():
        for c in range(3):
            ext[0, c] = out_x[c]
        copies = [coord_copy(zone) for zone in range(7)]
        for zone in range(7):
            copies[zone].wait()
        for c in range(3):
            ext[1, c] = zin[0, c] + float(CX if c == 0 else 0)
            merged = merge_zones(
                [zin[zone, c] for zone in range(1, 7)], jnp.zeros((8, LANES), jnp.float32)
            )
            ext[2, c] = merged + halo_offset(c)

    def pairs():
        def tile_step(tile, energy):
            at = pl.ds(pl.multiple_of(tile * LANES, LANES), LANES)
            beads = []
            for side in range(2):
                index = jnp.broadcast_to(pair_ref[side : side + 1, at], (8, LANES))
                lanes = index & (LANES - 1)
                in_own = index < LANES
                in_first = index < 2 * LANES
                beads.append(
                    [
                        jnp.where(
                            in_own,
                            take_lanes(ext[0, c], lanes),
                            jnp.where(
                                in_first,
                                take_lanes(ext[1, c], lanes),
                                take_lanes(ext[2, c], lanes),
                            ),
                        )
                        for c in range(3)
                    ]
                )
            on_first = [None] * 3
            on_second = [None] * 3
            for shift in range(8):
                gap = []
                for c in range(3):
                    other = beads[1][c]
                    if shift:
                        other = pltpu.roll(other, 8 - shift, 0)
                    gap.append(beads[0][c] - other)
                reach = jnp.maximum(weights[tile, shift] - dot3(gap, gap), 0.0)
                square = reach * reach
                energy = energy + square * reach
                for c in range(3):
                    push = square * gap[c]
                    back = pltpu.roll(push, shift, 0) if shift else push
                    on_first[c] = push if shift == 0 else on_first[c] + push
                    on_second[c] = -back if shift == 0 else on_second[c] - back
            for side, parts in enumerate((on_first, on_second)):
                start = pl.multiple_of(side * slots + tile * LANES, LANES)
                for c in range(3):
                    high = parts[c].astype(jnp.bfloat16).astype(jnp.float32)
                    fbuf[c * 8 : c * 8 + 8, pl.ds(start, LANES)] = high
                    fbuf[24 + c * 8 : 32 + c * 8, pl.ds(start, LANES)] = parts[c] - high
            return energy

        def group(number, energy):
            for inner in range(unroll):
                energy = tile_step(number * unroll + inner, energy)
            return energy

        return lax.fori_loop(0, tiles // unroll, group, jnp.zeros((8, LANES), jnp.float32))

    def scatter():
        values = fbuf[...].astype(jnp.bfloat16)
        halo = jnp.dot(values, table[:, LANES:], preferred_element_type=jnp.float32)
        halo = (6.0 * strength) * (halo[:24] + halo[24:])
        for half in (1, 0):
            for c in range(3):
                fout[half, c] = halo[c * 8 : c * 8 + 8, half * LANES : (half + 1) * LANES]
        copies = [force_copy(zone) for zone in range(7)]
        for zone in order:
            copies[zone].start()
        own = jnp.dot(values, table[:, :LANES], preferred_element_type=jnp.float32)
        own = (6.0 * strength) * (own[:24] + own[24:])
        for zone in range(7):
            copies[zone].wait()
        zero = jnp.zeros((8, LANES), jnp.float32)
        rows = []
        for c in range(3):
            merged = merge_zones([fin[zone, c] for zone in range(1, 7)], zero)
            rows.append(jnp.concatenate([fin[0, c], merged], axis=1))
        back = jnp.concatenate(rows, axis=0)
        high = back.astype(jnp.bfloat16).astype(jnp.float32)
        split = jnp.concatenate([high, back - high], axis=0).astype(jnp.bfloat16)
        added = jnp.dot(split, home[...], preferred_element_type=jnp.float32)
        total = own + added[:24] + added[24:]
        for c in range(3):
            force[c] = total[c * 8 : c * 8 + 8]

    def integrate():
        old = [out_x[c] for c in range(3)]
        half = [out_v[c] + (0.5 * time_step) * force[c] for c in range(3)]
        moved = [old[c] + time_step * half[c] for c in range(3)]
        directions = [unit[c] for c in range(3)]
        coupling = couple[...]
        vectors = [a - up(a) for a in moved]
        projected = dot3(directions, vectors)
        solved = expand(coupling, flags * root_half * (projected - rest))
        moved = apply_links(moved, directions, solved)
        for _ in range(NITER):
            vectors = [a - up(a) for a in moved]
            squared = dot3(vectors, vectors)
            target = jnp.sqrt(jnp.maximum(2.0 * rest * rest - squared, 0.25 * rest * rest))
            solved = expand(coupling, flags * root_half * (rest - target))
            moved = apply_links(moved, directions, solved)
        for c in range(3):
            out_v[c] = (moved[c] - old[c]) / time_step
            out_x[c] = moved[c]

    def step(number, carry):
        @pl.when(number > 0)
        def _():
            integrate()

        evaluate()
        prepare()

        @pl.when(number == 0)
        def _():
            build_tables()

        receive_coords()
        energy = pairs()
        scatter()

        @pl.when(number > 0)
        def _():
            speeds = [out_v[c] + (0.5 * time_step) * force[c] for c in range(3)]
            for c in range(3):
                out_v[c] = speeds[c]
            eacc[2 * (number - 1)] = strength * energy
            eacc[2 * (number - 1) + 1] = 0.5 * dot3(speeds, speeds)

        return carry

    lax.fori_loop(0, ITERS + 1, step, 0)

    total = jnp.zeros((8, LANES), jnp.float32)
    for row in range(2 * ITERS):
        line = jnp.sum(eacc[row], axis=0, keepdims=True)
        total = jnp.where(bead == row, line, total)
    eout[...] = total

    def energy_copy(number):
        return pltpu.make_async_remote_copy(
            src_ref=eout,
            dst_ref=ein.at[number],
            send_sem=esend_sem.at[number],
            recv_sem=erecv_sem.at[number],
            device_id=peer(sizes, number),
            device_id_type=MESH,
        )

    each_peer(sizes, lambda number: energy_copy(number).start())
    each_peer(sizes, lambda number: energy_copy(number).wait())
    if count <= 32:
        for number in range(1, count):
            total = total + ein[number]
    else:
        total = lax.fori_loop(1, count, lambda number, acc: acc + ein[number], total)
    beads = 8 * LANES * count
    summed = jnp.sum(total, axis=1, keepdims=True) / beads
    for row in range(ITERS):
        for column in range(2):
            at = 2 * row + column
            out_e[column : column + 1, row : row + 1] = summed[at : at + 1, :]


def finish(coords, speeds, sums, out_x, out_v, out_e):
    out_x[...] = coords[...]
    out_v[...] = speeds[...]
    out_e[...] = sums[...]


def on_device(sizes, positions, velocities, send_list, pair_list, constraint_flags):
    clusters = positions.shape[2]
    slots = pair_list.shape[1]
    tiles = slots // LANES
    count = sizes[0] * sizes[1] * sizes[2]
    unroll = max(u for u in range(1, 8) if tiles % u == 0)
    vmem = pl.BlockSpec(memory_space=pltpu.VMEM)
    f32 = jnp.float32
    coords, speeds, sums = pl.pallas_call(
        functools.partial(kernel, sizes, unroll),
        out_shape=(
            jax.ShapeDtypeStruct(positions.shape, f32),
            jax.ShapeDtypeStruct(velocities.shape, f32),
            jax.ShapeDtypeStruct((2, ITERS), f32),
        ),
        in_specs=[pl.BlockSpec(memory_space=pl.ANY)] * 5,
        out_specs=(vmem, vmem, vmem),
        scratch_shapes=[
            pltpu.VMEM(send_list.shape, jnp.int32),
            pltpu.VMEM((2, LANES), jnp.int32),
            pltpu.VMEM(pair_list.shape, jnp.int32),
            pltpu.VMEM(constraint_flags.shape, jnp.int32),
            pltpu.SemaphoreType.DMA((5,)),
            pltpu.VMEM((2 * slots, 3 * clusters), jnp.bfloat16),
            pltpu.VMEM((2 * clusters, clusters), jnp.bfloat16),
            pltpu.VMEM((tiles, 8, 8, LANES), f32),
            pltpu.VMEM((3, 3, 8, LANES), f32),
            pltpu.VMEM((7, 3, 8, LANES), f32),
            pltpu.VMEM((2, 3, 8, LANES), f32),
            pltpu.VMEM((2, 3, 8, LANES), f32),
            pltpu.VMEM((7, 3, 8, LANES), f32),
            pltpu.VMEM((48, 2 * slots), f32),
            pltpu.VMEM((3, 8, LANES), f32),
            pltpu.VMEM((3, 8, LANES), f32),
            pltpu.VMEM((8, LANES), f32),
            pltpu.VMEM((2 * ITERS, 8, LANES), f32),
            pltpu.VMEM((8, LANES), f32),
            pltpu.VMEM((count, 8, LANES), f32),
            pltpu.SemaphoreType.DMA((7,)),
            pltpu.SemaphoreType.DMA((7,)),
            pltpu.SemaphoreType.DMA((7,)),
            pltpu.SemaphoreType.DMA((7,)),
            pltpu.SemaphoreType.DMA((count,)),
            pltpu.SemaphoreType.DMA((count,)),
        ],
        compiler_params=pltpu.CompilerParams(collective_id=0, has_side_effects=True),
    )(positions, velocities, send_list, pair_list, constraint_flags)
    results = (coords, speeds, sums)
    coords, speeds, sums = pl.pallas_call(
        finish,
        out_shape=tuple(jax.ShapeDtypeStruct(r.shape, f32) for r in results),
        in_specs=[vmem] * 3,
        out_specs=(vmem, vmem, vmem),
    )(*results)
    return coords, speeds, sums.T


def solution(mesh):
    sizes = tuple(mesh.shape[axis] for axis in AXES)
    split = ("runs", "gx", "gy", "gz")
    return jax.shard_map(
        functools.partial(on_device, sizes),
        mesh=mesh,
        in_specs=(
            P(None, None, split),
            P(None, None, split),
            P(split),
            P(None, split),
            P(None, split),
        ),
        out_specs=(P(None, None, split), P(None, None, split), P("runs", None)),
        check_vma=False,
    )
```

```python
import functools
import itertools

import jax
import jax.numpy as jnp
from jax import lax
from jax.experimental import pallas as pl
from jax.experimental.pallas import tpu as pltpu
from jax.sharding import PartitionSpec as P

CX = 1
CY = 8
CZ = 16
ITERS = 3
NORDER = 4
NITER = 1

MESH = pl.DeviceIdType.MESH
AXES = ("gx", "gy", "gz")
LANES = 128
WIDTH = LANES // 8

time_step = 0.02
strength = 2.0
root_half = 0.7071067811865476
zone_list = ((1, 0, 0), (0, 1, 0), (0, 0, 1), (1, 1, 0), (1, 0, 1), (0, 1, 1), (1, 1, 1))


def zone_sizes():
    return tuple(
        (CX if d[0] == 0 else 1) * (CY if d[1] == 0 else 1) * (CZ if d[2] == 0 else 1)
        for d in zone_list
    )


def zone_spans():
    spans = []
    position = 0
    for size in zone_sizes()[1:]:
        spans.append((position, position + size))
        position += size
    return spans


def neighbour(sizes, direction, sign):
    ids = {}
    for axis, size, step in zip(AXES, sizes, direction):
        if step:
            ids[axis] = lax.rem(lax.axis_index(axis) + (size + sign * step), size)
    return ids


def peer(sizes, number):
    _, ny, nz = sizes
    steps = (number // (ny * nz), (number // nz) % ny, number % nz)
    return {
        axis: lax.rem(lax.axis_index(axis) + step, size)
        for axis, size, step in zip(AXES, sizes, steps)
    }


def each_peer(sizes, body):
    count = sizes[0] * sizes[1] * sizes[2]
    if count <= 32:
        for number in range(1, count):
            body(number)
    else:

        def step(number, carry):
            body(number)
            return carry

        lax.fori_loop(1, count, step, 0)


def up(value):
    return pltpu.roll(value, 7, 0)


def down(value):
    return pltpu.roll(value, 1, 0)


def dot3(a, b):
    return a[0] * b[0] + a[1] * b[1] + a[2] * b[2]


def expand(coupling, source):
    coupling_down = down(coupling)
    series = source
    result = source
    for _ in range(NORDER):
        series = coupling_down * down(series) + coupling * up(series)
        result = result + series
    return result


def apply_links(coords, directions, solution):
    scaled = root_half * solution
    moved = []
    for c in range(3):
        shift = directions[c] * scaled
        moved.append(coords[c] - shift + down(shift))
    return moved


def take_lanes(value, lanes):
    return jnp.take_along_axis(value, lanes, axis=1, mode="promise_in_bounds")


def pack_zone(value, lanes):
    bead = lax.broadcasted_iota(jnp.int32, (8, LANES), 0)
    lane = lax.broadcasted_iota(jnp.int32, (8, LANES), 1)
    chosen = jnp.where(lane // WIDTH == bead, take_lanes(value, lanes), 0.0)
    return jnp.sum(chosen, axis=0, keepdims=True)


def merge_zones(rows):
    bead = lax.broadcasted_iota(jnp.int32, (8, LANES), 0)
    lane = lax.broadcasted_iota(jnp.int32, (8, LANES), 1)
    merged = jnp.zeros((8, LANES), jnp.float32)
    for row, (low, high) in zip(rows, zone_spans()):
        lanes = bead * WIDTH + jnp.clip(lane - low, 0, WIDTH - 1)
        spread = take_lanes(jnp.broadcast_to(row, (8, LANES)), lanes)
        merged = jnp.where((lane >= low) & (lane < high), spread, merged)
    return merged


def halo_offset(c):
    lane = lax.broadcasted_iota(jnp.int32, (8, LANES), 1)
    offset = jnp.zeros((8, LANES), jnp.float32)
    for number, (low, high) in enumerate(zone_spans()):
        if zone_list[number + 1][c]:
            offset = jnp.where(
                (lane >= low) & (lane < high), float((CX, CY, CZ)[c]), offset
            )
    return offset


def kernel(
    sizes,
    unroll,
    pos_hbm,
    vel_hbm,
    send_hbm,
    pair_hbm,
    flag_hbm,
    out_x,
    out_v,
    out_e,
    send_flat,
    send_ref,
    pair_ref,
    flag_ref,
    load_sem,
    table,
    home,
    weights,
    ext,
    picks,
    zin,
    zmsg,
    cout,
    cmsg,
    fout,
    fmsg,
    fin,
    finmsg,
    fbuf,
    force,
    unit,
    couple,
    eacc,
    eout,
    ein,
    send_sem,
    recv_sem,
    fsend_sem,
    frecv_sem,
    esend_sem,
    erecv_sem,
):
    slots = pair_ref.shape[1]
    tiles = slots // LANES
    bead = lax.broadcasted_iota(jnp.int32, (8, LANES), 0)
    count = sizes[0] * sizes[1] * sizes[2]
    pad_index = 2 * LANES + zone_spans()[-1][1]

    barrier = pltpu.get_barrier_semaphore()

    def greet(number):
        pl.semaphore_signal(barrier, inc=1, device_id=peer(sizes, number), device_id_type=MESH)

    each_peer(sizes, greet)

    loads = [
        pltpu.make_async_copy(source, target, load_sem.at[number])
        for number, (source, target) in enumerate(
            (
                (pos_hbm, out_x),
                (send_hbm, send_flat),
                (pair_hbm, pair_ref),
                (flag_hbm, flag_ref),
                (vel_hbm, out_v),
            )
        )
    ]
    for load in loads:
        load.start()
    for load in loads:
        load.wait()
    small = send_flat.shape[0] - LANES
    send_ref[0:1, :] = send_flat[0:LANES].reshape(1, LANES)
    send_ref[1:2, :] = jnp.concatenate(
        [send_flat[LANES:], jnp.zeros((LANES - small,), jnp.int32)]
    ).reshape(1, LANES)
    flags = jnp.concatenate(
        [flag_ref[...].astype(jnp.float32), jnp.zeros((1, LANES), jnp.float32)], axis=0
    )
    flags_up = up(flags)
    first = [out_x[c] for c in range(3)]
    links = [a - up(a) for a in first]
    rest = jnp.sqrt(dot3(links, links))

    lane = lax.broadcasted_iota(jnp.int32, (8, LANES), 1)
    listed = jnp.broadcast_to(send_ref[1:2, :], (8, LANES))
    for number, (low, _) in enumerate(zone_spans()):
        picks[number] = take_lanes(listed, low + lane % WIDTH)

    pl.semaphore_wait(barrier, count - 1)

    def coord_copy(zone):
        return pltpu.make_async_remote_copy(
            src_ref=cmsg.at[zone - 1] if zone else cout,
            dst_ref=zmsg.at[zone - 1] if zone else zin,
            send_sem=send_sem.at[zone],
            recv_sem=recv_sem.at[zone],
            device_id=neighbour(sizes, zone_list[zone], -1),
            device_id_type=MESH,
        )

    def force_copy(zone):
        return pltpu.make_async_remote_copy(
            src_ref=fmsg.at[zone - 1] if zone else fout,
            dst_ref=finmsg.at[zone - 1] if zone else fin,
            send_sem=fsend_sem.at[zone],
            recv_sem=frecv_sem.at[zone],
            device_id=neighbour(sizes, zone_list[zone], 1),
            device_id_type=MESH,
        )

    order = (3, 0, 6, 4, 1, 5, 2)
    lane = lax.broadcasted_iota(jnp.int32, (8, LANES), 1)
    inside = [low + lane % WIDTH for low, _ in zone_spans()]

    def evaluate():
        lanes = jnp.broadcast_to(send_ref[0:1, :], (8, LANES))
        for zone in order:
            for c in range(3):
                if zone:
                    cmsg[zone - 1, c : c + 1, :] = pack_zone(out_x[c], picks[zone - 1])
                else:
                    cout[c] = take_lanes(out_x[c], lanes)
            coord_copy(zone).start()

    def prepare():
        old = [out_x[c] for c in range(3)]
        vectors = [a - up(a) for a in old]
        length = jnp.maximum(jnp.sqrt(dot3(vectors, vectors)), 0.2)
        directions = [a / length for a in vectors]
        for c in range(3):
            unit[c] = directions[c]
        couple[...] = 0.5 * dot3(directions, [up(a) for a in directions]) * flags * flags_up

    def build_tables():
        lane = lax.broadcasted_iota(jnp.int32, (LANES, LANES), 1)
        for half in range(2):
            rows = jnp.broadcast_to(send_ref[half : half + 1, :], (LANES, LANES)).T
            home[half * LANES : (half + 1) * LANES, :] = (
                (rows == lane).astype(jnp.float32).astype(jnp.bfloat16)
            )

        def build(tile, carry):
            at = pl.ds(pl.multiple_of(tile * LANES, LANES), LANES)
            for side in range(2):
                rows = jnp.broadcast_to(pair_ref[side : side + 1, at], (LANES, LANES)).T
                start = pl.multiple_of(side * slots + tile * LANES, LANES)
                for block in range(3):
                    table[pl.ds(start, LANES), block * LANES : (block + 1) * LANES] = (
                        (rows == lane + block * LANES).astype(jnp.float32).astype(jnp.bfloat16)
                    )
            one = jnp.broadcast_to(pair_ref[0:1, at], (8, LANES))
            two = jnp.broadcast_to(pair_ref[1:2, at], (8, LANES))
            for shift in range(8):
                use = one != two
                if shift:
                    use = use | (bead < 8 - shift)
                use = use & (one != pad_index)
                weights[tile, shift] = use.astype(jnp.float32)
            return carry

        lax.fori_loop(0, tiles, build, 0)

    def receive_coords():
        for c in range(3):
            ext[0, c] = out_x[c]
        copies = [coord_copy(zone) for zone in range(7)]
        for zone in range(7):
            copies[zone].wait()
        for c in range(3):
            ext[1, c] = zin[c] + float(CX if c == 0 else 0)
            merged = merge_zones([zmsg[number, c : c + 1, :] for number in range(6)])
            ext[2, c] = merged + halo_offset(c)

    def pairs():
        def tile_step(tile, energy):
            at = pl.ds(pl.multiple_of(tile * LANES, LANES), LANES)
            beads = []
            for side in range(2):
                index = jnp.broadcast_to(pair_ref[side : side + 1, at], (8, LANES))
                lanes = index & (LANES - 1)
                in_own = index < LANES
                in_first = index < 2 * LANES
                beads.append(
                    [
                        jnp.where(
                            in_own,
                            take_lanes(ext[0, c], lanes),
                            jnp.where(
                                in_first,
                                take_lanes(ext[1, c], lanes),
                                take_lanes(ext[2, c], lanes),
                            ),
                        )
                        for c in range(3)
                    ]
                )
            on_first = [None] * 3
            on_second = [None] * 3
            for shift in range(8):
                gap = []
                for c in range(3):
                    other = beads[1][c]
                    if shift:
                        other = pltpu.roll(other, 8 - shift, 0)
                    gap.append(beads[0][c] - other)
                reach = jnp.maximum(weights[tile, shift] - dot3(gap, gap), 0.0)
                square = reach * reach
                energy = energy + square * reach
                for c in range(3):
                    push = square * gap[c]
                    back = pltpu.roll(push, shift, 0) if shift else push
                    on_first[c] = push if shift == 0 else on_first[c] + push
                    on_second[c] = -back if shift == 0 else on_second[c] - back
            for side, parts in enumerate((on_first, on_second)):
                start = pl.multiple_of(side * slots + tile * LANES, LANES)
                for c in range(3):
                    high = parts[c].astype(jnp.bfloat16).astype(jnp.float32)
                    fbuf[c * 8 : c * 8 + 8, pl.ds(start, LANES)] = high
                    fbuf[24 + c * 8 : 32 + c * 8, pl.ds(start, LANES)] = parts[c] - high
            return energy

        def group(number, energy):
            for inner in range(unroll):
                energy = tile_step(number * unroll + inner, energy)
            return energy

        return lax.fori_loop(0, tiles // unroll, group, jnp.zeros((8, LANES), jnp.float32))

    def scatter():
        values = fbuf[...].astype(jnp.bfloat16)
        halo = jnp.dot(values, table[:, LANES:], preferred_element_type=jnp.float32)
        halo = (6.0 * strength) * (halo[:24] + halo[24:])
        copies = [force_copy(zone) for zone in range(7)]
        for zone in order:
            for c in range(3):
                rows = halo[c * 8 : c * 8 + 8]
                if zone:
                    fmsg[zone - 1, c : c + 1, :] = pack_zone(rows[:, LANES:], inside[zone - 1])
                else:
                    fout[c] = rows[:, :LANES]
            copies[zone].start()
        own = jnp.dot(values, table[:, :LANES], preferred_element_type=jnp.float32)
        own = (6.0 * strength) * (own[:24] + own[24:])
        for zone in range(7):
            copies[zone].wait()
        rows = []
        for c in range(3):
            merged = merge_zones([finmsg[number, c : c + 1, :] for number in range(6)])
            rows.append(jnp.concatenate([fin[c], merged], axis=1))
        back = jnp.concatenate(rows, axis=0)
        high = back.astype(jnp.bfloat16).astype(jnp.float32)
        split = jnp.concatenate([high, back - high], axis=0).astype(jnp.bfloat16)
        added = jnp.dot(split, home[...], preferred_element_type=jnp.float32)
        total = own + added[:24] + added[24:]
        for c in range(3):
            force[c] = total[c * 8 : c * 8 + 8]

    def integrate():
        old = [out_x[c] for c in range(3)]
        half = [out_v[c] + (0.5 * time_step) * force[c] for c in range(3)]
        moved = [old[c] + time_step * half[c] for c in range(3)]
        directions = [unit[c] for c in range(3)]
        coupling = couple[...]
        vectors = [a - up(a) for a in moved]
        projected = dot3(directions, vectors)
        solved = expand(coupling, flags * root_half * (projected - rest))
        moved = apply_links(moved, directions, solved)
        for _ in range(NITER):
            vectors = [a - up(a) for a in moved]
            squared = dot3(vectors, vectors)
            target = jnp.sqrt(jnp.maximum(2.0 * rest * rest - squared, 0.25 * rest * rest))
            solved = expand(coupling, flags * root_half * (rest - target))
            moved = apply_links(moved, directions, solved)
        for c in range(3):
            out_v[c] = (moved[c] - old[c]) / time_step
            out_x[c] = moved[c]

    def step(number, carry):
        @pl.when(number > 0)
        def _():
            integrate()

        evaluate()
        prepare()

        @pl.when(number == 0)
        def _():
            build_tables()

        receive_coords()
        energy = pairs()
        scatter()

        @pl.when(number > 0)
        def _():
            speeds = [out_v[c] + (0.5 * time_step) * force[c] for c in range(3)]
            for c in range(3):
                out_v[c] = speeds[c]
            eacc[2 * (number - 1)] = strength * energy
            eacc[2 * (number - 1) + 1] = 0.5 * dot3(speeds, speeds)

        return carry

    lax.fori_loop(0, ITERS + 1, step, 0)

    total = jnp.zeros((8, LANES), jnp.float32)
    for row in range(2 * ITERS):
        line = jnp.sum(eacc[row], axis=0, keepdims=True)
        total = jnp.where(bead == row, line, total)
    eout[...] = total

    def energy_copy(number):
        return pltpu.make_async_remote_copy(
            src_ref=eout,
            dst_ref=ein.at[number],
            send_sem=esend_sem.at[number],
            recv_sem=erecv_sem.at[number],
            device_id=peer(sizes, number),
            device_id_type=MESH,
        )

    each_peer(sizes, lambda number: energy_copy(number).start())
    each_peer(sizes, lambda number: energy_copy(number).wait())
    if count <= 32:
        for number in range(1, count):
            total = total + ein[number]
    else:
        total = lax.fori_loop(1, count, lambda number, acc: acc + ein[number], total)
    beads = 8 * LANES * count
    summed = jnp.sum(total, axis=1, keepdims=True) / beads
    for row in range(ITERS):
        for column in range(2):
            at = 2 * row + column
            out_e[column : column + 1, row : row + 1] = summed[at : at + 1, :]


def finish(coords, speeds, sums, out_x, out_v, out_e):
    out_x[...] = coords[...]
    out_v[...] = speeds[...]
    out_e[...] = sums[...]


def on_device(sizes, positions, velocities, send_list, pair_list, constraint_flags):
    clusters = positions.shape[2]
    slots = pair_list.shape[1]
    tiles = slots // LANES
    count = sizes[0] * sizes[1] * sizes[2]
    unroll = max(u for u in range(1, 8) if tiles % u == 0)
    vmem = pl.BlockSpec(memory_space=pltpu.VMEM)
    f32 = jnp.float32
    coords, speeds, sums = pl.pallas_call(
        functools.partial(kernel, sizes, unroll),
        out_shape=(
            jax.ShapeDtypeStruct(positions.shape, f32),
            jax.ShapeDtypeStruct(velocities.shape, f32),
            jax.ShapeDtypeStruct((2, ITERS), f32),
        ),
        in_specs=[pl.BlockSpec(memory_space=pl.ANY)] * 5,
        out_specs=(vmem, vmem, vmem),
        scratch_shapes=[
            pltpu.VMEM(send_list.shape, jnp.int32),
            pltpu.VMEM((2, LANES), jnp.int32),
            pltpu.VMEM(pair_list.shape, jnp.int32),
            pltpu.VMEM(constraint_flags.shape, jnp.int32),
            pltpu.SemaphoreType.DMA((5,)),
            pltpu.VMEM((2 * slots, 3 * clusters), jnp.bfloat16),
            pltpu.VMEM((2 * clusters, clusters), jnp.bfloat16),
            pltpu.VMEM((tiles, 8, 8, LANES), f32),
            pltpu.VMEM((3, 3, 8, LANES), f32),
            pltpu.VMEM((6, 8, LANES), jnp.int32),
            pltpu.VMEM((3, 8, LANES), f32),
            pltpu.VMEM((6, 3, LANES), f32),
            pltpu.VMEM((3, 8, LANES), f32),
            pltpu.VMEM((6, 3, LANES), f32),
            pltpu.VMEM((3, 8, LANES), f32),
            pltpu.VMEM((6, 3, LANES), f32),
            pltpu.VMEM((3, 8, LANES), f32),
            pltpu.VMEM((6, 3, LANES), f32),
            pltpu.VMEM((48, 2 * slots), f32),
            pltpu.VMEM((3, 8, LANES), f32),
            pltpu.VMEM((3, 8, LANES), f32),
            pltpu.VMEM((8, LANES), f32),
            pltpu.VMEM((2 * ITERS, 8, LANES), f32),
            pltpu.VMEM((8, LANES), f32),
            pltpu.VMEM((count, 8, LANES), f32),
            pltpu.SemaphoreType.DMA((7,)),
            pltpu.SemaphoreType.DMA((7,)),
            pltpu.SemaphoreType.DMA((7,)),
            pltpu.SemaphoreType.DMA((7,)),
            pltpu.SemaphoreType.DMA((count,)),
            pltpu.SemaphoreType.DMA((count,)),
        ],
        compiler_params=pltpu.CompilerParams(collective_id=0, has_side_effects=True),
    )(positions, velocities, send_list, pair_list, constraint_flags)
    results = (coords, speeds, sums)
    coords, speeds, sums = pl.pallas_call(
        finish,
        out_shape=tuple(jax.ShapeDtypeStruct(r.shape, f32) for r in results),
        in_specs=[vmem] * 3,
        out_specs=(vmem, vmem, vmem),
    )(*results)
    return coords, speeds, sums.T


def solution(mesh):
    sizes = tuple(mesh.shape[axis] for axis in AXES)
    split = ("runs", "gx", "gy", "gz")
    return jax.shard_map(
        functools.partial(on_device, sizes),
        mesh=mesh,
        in_specs=(
            P(None, None, split),
            P(None, None, split),
            P(split),
            P(None, split),
            P(None, split),
        ),
        out_specs=(P(None, None, split), P(None, None, split), P("runs", None)),
        check_vma=False,
    )
```

```python
import functools
import itertools

import jax
import jax.numpy as jnp
from jax import lax
from jax.experimental import pallas as pl
from jax.experimental.pallas import tpu as pltpu
from jax.sharding import PartitionSpec as P

CX = 1
CY = 8
CZ = 16
ITERS = 3
NORDER = 4
NITER = 1

MESH = pl.DeviceIdType.MESH
AXES = ("gx", "gy", "gz")
LANES = 128
WIDTH = LANES // 8

time_step = 0.02
strength = 2.0
root_half = 0.7071067811865476
zone_list = ((1, 0, 0), (0, 1, 0), (0, 0, 1), (1, 1, 0), (1, 0, 1), (0, 1, 1), (1, 1, 1))


def zone_sizes():
    return tuple(
        (CX if d[0] == 0 else 1) * (CY if d[1] == 0 else 1) * (CZ if d[2] == 0 else 1)
        for d in zone_list
    )


def zone_spans():
    spans = []
    position = 0
    for size in zone_sizes()[1:]:
        spans.append((position, position + size))
        position += size
    return spans


def neighbour(sizes, direction, sign):
    ids = {}
    for axis, size, step in zip(AXES, sizes, direction):
        if step:
            ids[axis] = lax.rem(lax.axis_index(axis) + (size + sign * step), size)
    return ids


def peer(sizes, number):
    _, ny, nz = sizes
    steps = (number // (ny * nz), (number // nz) % ny, number % nz)
    return {
        axis: lax.rem(lax.axis_index(axis) + step, size)
        for axis, size, step in zip(AXES, sizes, steps)
    }


def each_peer(sizes, body):
    count = sizes[0] * sizes[1] * sizes[2]
    if count <= 32:
        for number in range(1, count):
            body(number)
    else:

        def step(number, carry):
            body(number)
            return carry

        lax.fori_loop(1, count, step, 0)


def up(value):
    return pltpu.roll(value, 7, 0)


def down(value):
    return pltpu.roll(value, 1, 0)


def dot3(a, b):
    return a[0] * b[0] + a[1] * b[1] + a[2] * b[2]


def expand(coupling, source):
    coupling_down = down(coupling)
    series = source
    result = source
    for _ in range(NORDER):
        series = coupling_down * down(series) + coupling * up(series)
        result = result + series
    return result


def apply_links(coords, directions, solution):
    scaled = root_half * solution
    moved = []
    for c in range(3):
        shift = directions[c] * scaled
        moved.append(coords[c] - shift + down(shift))
    return moved


def take_lanes(value, lanes):
    return jnp.take_along_axis(value, lanes, axis=1, mode="promise_in_bounds")


def pack_zone(value, lanes):
    bead = lax.broadcasted_iota(jnp.int32, (8, LANES), 0)
    lane = lax.broadcasted_iota(jnp.int32, (8, LANES), 1)
    chosen = jnp.where(lane // WIDTH == bead, take_lanes(value, lanes), 0.0)
    return jnp.sum(chosen, axis=0, keepdims=True)


def merge_zones(rows):
    bead = lax.broadcasted_iota(jnp.int32, (8, LANES), 0)
    lane = lax.broadcasted_iota(jnp.int32, (8, LANES), 1)
    merged = jnp.zeros((8, LANES), jnp.float32)
    for row, (low, high) in zip(rows, zone_spans()):
        lanes = bead * WIDTH + jnp.clip(lane - low, 0, WIDTH - 1)
        spread = take_lanes(jnp.broadcast_to(row, (8, LANES)), lanes)
        merged = jnp.where((lane >= low) & (lane < high), spread, merged)
    return merged


def halo_offset(c):
    lane = lax.broadcasted_iota(jnp.int32, (8, LANES), 1)
    offset = jnp.zeros((8, LANES), jnp.float32)
    for number, (low, high) in enumerate(zone_spans()):
        if zone_list[number + 1][c]:
            offset = jnp.where(
                (lane >= low) & (lane < high), float((CX, CY, CZ)[c]), offset
            )
    return offset


def kernel(
    sizes,
    unroll,
    pos_hbm,
    vel_hbm,
    send_hbm,
    pair_hbm,
    flag_hbm,
    out_x,
    out_v,
    out_e,
    send_flat,
    send_ref,
    pair_ref,
    flag_ref,
    load_sem,
    table,
    home,
    weights,
    ext,
    picks,
    zin,
    zmsg,
    cout,
    cmsg,
    fout,
    fmsg,
    fin,
    finmsg,
    fbuf,
    force,
    unit,
    couple,
    eacc,
    eout,
    ein,
    send_sem,
    recv_sem,
    fsend_sem,
    frecv_sem,
    esend_sem,
    erecv_sem,
):
    slots = pair_ref.shape[1]
    tiles = slots // LANES
    bead = lax.broadcasted_iota(jnp.int32, (8, LANES), 0)
    count = sizes[0] * sizes[1] * sizes[2]
    pad_index = 2 * LANES + zone_spans()[-1][1]

    barrier = pltpu.get_barrier_semaphore()

    def greet(number):
        pl.semaphore_signal(barrier, inc=1, device_id=peer(sizes, number), device_id_type=MESH)

    each_peer(sizes, greet)

    loads = [
        pltpu.make_async_copy(source, target, load_sem.at[number])
        for number, (source, target) in enumerate(
            (
                (pos_hbm, out_x),
                (send_hbm, send_flat),
                (pair_hbm, pair_ref),
                (flag_hbm, flag_ref),
                (vel_hbm, out_v),
            )
        )
    ]
    for load in loads:
        load.start()
    for load in loads:
        load.wait()
    small = send_flat.shape[0] - LANES
    send_ref[0:1, :] = send_flat[0:LANES].reshape(1, LANES)
    send_ref[1:2, :] = jnp.concatenate(
        [send_flat[LANES:], jnp.zeros((LANES - small,), jnp.int32)]
    ).reshape(1, LANES)
    flags = jnp.concatenate(
        [flag_ref[...].astype(jnp.float32), jnp.zeros((1, LANES), jnp.float32)], axis=0
    )
    flags_up = up(flags)
    first = [out_x[c] for c in range(3)]
    links = [a - up(a) for a in first]
    rest = jnp.sqrt(dot3(links, links))

    lane = lax.broadcasted_iota(jnp.int32, (8, LANES), 1)
    listed = jnp.broadcast_to(send_ref[1:2, :], (8, LANES))
    for number, (low, _) in enumerate(zone_spans()):
        picks[number] = take_lanes(listed, low + lane % WIDTH)

    pl.semaphore_wait(barrier, count - 1)

    def coord_copy(zone):
        return pltpu.make_async_remote_copy(
            src_ref=cmsg.at[zone - 1] if zone else cout,
            dst_ref=zmsg.at[zone - 1] if zone else zin,
            send_sem=send_sem.at[zone],
            recv_sem=recv_sem.at[zone],
            device_id=neighbour(sizes, zone_list[zone], -1),
            device_id_type=MESH,
        )

    def force_copy(zone):
        return pltpu.make_async_remote_copy(
            src_ref=fmsg.at[zone - 1] if zone else fout,
            dst_ref=finmsg.at[zone - 1] if zone else fin,
            send_sem=fsend_sem.at[zone],
            recv_sem=frecv_sem.at[zone],
            device_id=neighbour(sizes, zone_list[zone], 1),
            device_id_type=MESH,
        )

    order = (3, 0, 6, 4, 1, 5, 2)
    lane = lax.broadcasted_iota(jnp.int32, (8, LANES), 1)
    inside = [low + lane % WIDTH for low, _ in zone_spans()]

    def evaluate():
        lanes = jnp.broadcast_to(send_ref[0:1, :], (8, LANES))
        for zone in order:
            for c in range(3):
                if zone:
                    cmsg[zone - 1, c : c + 1, :] = pack_zone(out_x[c], picks[zone - 1])
                else:
                    cout[c] = take_lanes(out_x[c], lanes)
            coord_copy(zone).start()

    def prepare():
        old = [out_x[c] for c in range(3)]
        vectors = [a - up(a) for a in old]
        length = jnp.maximum(jnp.sqrt(dot3(vectors, vectors)), 0.2)
        directions = [a / length for a in vectors]
        for c in range(3):
            unit[c] = directions[c]
        couple[...] = 0.5 * dot3(directions, [up(a) for a in directions]) * flags * flags_up

    def build_tables():
        lane = lax.broadcasted_iota(jnp.int32, (LANES, LANES), 1)
        for half in range(2):
            rows = jnp.broadcast_to(send_ref[half : half + 1, :], (LANES, LANES)).T
            home[half * LANES : (half + 1) * LANES, :] = (
                (rows == lane).astype(jnp.float32).astype(jnp.bfloat16)
            )

        def build(tile, carry):
            at = pl.ds(pl.multiple_of(tile * LANES, LANES), LANES)
            for side in range(2):
                rows = jnp.broadcast_to(pair_ref[side : side + 1, at], (LANES, LANES)).T
                start = pl.multiple_of(side * slots + tile * LANES, LANES)
                for block in range(3):
                    table[pl.ds(start, LANES), block * LANES : (block + 1) * LANES] = (
                        (rows == lane + block * LANES).astype(jnp.float32).astype(jnp.bfloat16)
                    )
            one = jnp.broadcast_to(pair_ref[0:1, at], (8, LANES))
            two = jnp.broadcast_to(pair_ref[1:2, at], (8, LANES))
            for shift in range(8):
                use = one != two
                if shift:
                    use = use | (bead < 8 - shift)
                use = use & (one != pad_index)
                weights[tile, shift] = use.astype(jnp.float32)
            return carry

        lax.fori_loop(0, tiles, build, 0)

    def receive_coords():
        for c in range(3):
            ext[0, c] = out_x[c]
        copies = [coord_copy(zone) for zone in range(7)]
        for zone in range(7):
            copies[zone].wait()
        for c in range(3):
            ext[1, c] = zin[c] + float(CX if c == 0 else 0)
            merged = merge_zones([zmsg[number, c : c + 1, :] for number in range(6)])
            ext[2, c] = merged + halo_offset(c)

    def pairs():
        def tile_step(tile, energy):
            at = pl.ds(pl.multiple_of(tile * LANES, LANES), LANES)
            beads = []
            for side in range(2):
                index = jnp.broadcast_to(pair_ref[side : side + 1, at], (8, LANES))
                lanes = index & (LANES - 1)
                in_own = index < LANES
                in_first = index < 2 * LANES
                beads.append(
                    [
                        jnp.where(
                            in_own,
                            take_lanes(ext[0, c], lanes),
                            jnp.where(
                                in_first,
                                take_lanes(ext[1, c], lanes),
                                take_lanes(ext[2, c], lanes),
                            ),
                        )
                        for c in range(3)
                    ]
                )
            on_first = [None] * 3
            on_second = [None] * 3
            for shift in range(8):
                gap = []
                for c in range(3):
                    other = beads[1][c]
                    if shift:
                        other = pltpu.roll(other, 8 - shift, 0)
                    gap.append(beads[0][c] - other)
                reach = jnp.maximum(weights[tile, shift] - dot3(gap, gap), 0.0)
                square = reach * reach
                energy = energy + square * reach
                for c in range(3):
                    push = square * gap[c]
                    back = pltpu.roll(push, shift, 0) if shift else push
                    on_first[c] = push if shift == 0 else on_first[c] + push
                    on_second[c] = -back if shift == 0 else on_second[c] - back
            for side, parts in enumerate((on_first, on_second)):
                start = pl.multiple_of(side * slots + tile * LANES, LANES)
                for c in range(3):
                    high = parts[c].astype(jnp.bfloat16).astype(jnp.float32)
                    fbuf[c * 8 : c * 8 + 8, pl.ds(start, LANES)] = high
                    fbuf[24 + c * 8 : 32 + c * 8, pl.ds(start, LANES)] = parts[c] - high
            return energy

        def group(number, energy):
            for inner in range(unroll):
                energy = tile_step(number * unroll + inner, energy)
            return energy

        return lax.fori_loop(0, tiles // unroll, group, jnp.zeros((8, LANES), jnp.float32))

    def scatter():
        values = fbuf[...].astype(jnp.bfloat16)
        halo = jnp.dot(values, table[:, LANES:], preferred_element_type=jnp.float32)
        halo = (6.0 * strength) * (halo[:24] + halo[24:])
        copies = [force_copy(zone) for zone in range(7)]
        for zone in order:
            for c in range(3):
                rows = halo[c * 8 : c * 8 + 8]
                if zone:
                    fmsg[zone - 1, c : c + 1, :] = pack_zone(rows[:, LANES:], inside[zone - 1])
                else:
                    fout[c] = rows[:, :LANES]
            copies[zone].start()
        own = jnp.dot(values, table[:, :LANES], preferred_element_type=jnp.float32)
        own = (6.0 * strength) * (own[:24] + own[24:])
        for zone in range(7):
            copies[zone].wait()
        rows = []
        for c in range(3):
            merged = merge_zones([finmsg[number, c : c + 1, :] for number in range(6)])
            rows.append(jnp.concatenate([fin[c], merged], axis=1))
        back = jnp.concatenate(rows, axis=0)
        high = back.astype(jnp.bfloat16).astype(jnp.float32)
        split = jnp.concatenate([high, back - high], axis=0).astype(jnp.bfloat16)
        added = jnp.dot(split, home[...], preferred_element_type=jnp.float32)
        total = own + added[:24] + added[24:]
        for c in range(3):
            force[c] = total[c * 8 : c * 8 + 8]

    def integrate():
        old = [out_x[c] for c in range(3)]
        half = [out_v[c] + (0.5 * time_step) * force[c] for c in range(3)]
        moved = [old[c] + time_step * half[c] for c in range(3)]
        directions = [unit[c] for c in range(3)]
        coupling = couple[...]
        vectors = [a - up(a) for a in moved]
        projected = dot3(directions, vectors)
        solved = expand(coupling, flags * root_half * (projected - rest))
        moved = apply_links(moved, directions, solved)
        for _ in range(NITER):
            vectors = [a - up(a) for a in moved]
            squared = dot3(vectors, vectors)
            target = jnp.sqrt(jnp.maximum(2.0 * rest * rest - squared, 0.25 * rest * rest))
            solved = expand(coupling, flags * root_half * (rest - target))
            moved = apply_links(moved, directions, solved)
        for c in range(3):
            out_v[c] = (moved[c] - old[c]) / time_step
            out_x[c] = moved[c]

    def step(number, carry):
        @pl.when(number > 0)
        def _():
            integrate()

        evaluate()
        prepare()

        @pl.when(number == 0)
        def _():
            build_tables()

        receive_coords()
        energy = pairs()
        scatter()

        @pl.when(number > 0)
        def _():
            speeds = [out_v[c] + (0.5 * time_step) * force[c] for c in range(3)]
            for c in range(3):
                out_v[c] = speeds[c]
            eacc[2 * (number - 1)] = strength * energy
            eacc[2 * (number - 1) + 1] = 0.5 * dot3(speeds, speeds)

        return carry

    lax.fori_loop(0, ITERS + 1, step, 0)

    total = jnp.zeros((8, LANES), jnp.float32)
    for row in range(2 * ITERS):
        line = jnp.sum(eacc[row], axis=0, keepdims=True)
        total = jnp.where(bead == row, line, total)
    eout[...] = total

    def energy_copy(number):
        return pltpu.make_async_remote_copy(
            src_ref=eout,
            dst_ref=ein.at[number],
            send_sem=esend_sem.at[number],
            recv_sem=erecv_sem.at[number],
            device_id=peer(sizes, number),
            device_id_type=MESH,
        )

    each_peer(sizes, lambda number: energy_copy(number).start())
    each_peer(sizes, lambda number: energy_copy(number).wait())
    if count <= 32:
        for number in range(1, count):
            total = total + ein[number]
    else:
        total = lax.fori_loop(1, count, lambda number, acc: acc + ein[number], total)
    beads = 8 * LANES * count
    summed = jnp.sum(total, axis=1, keepdims=True) / beads
    for row in range(ITERS):
        for column in range(2):
            at = 2 * row + column
            out_e[column : column + 1, row : row + 1] = summed[at : at + 1, :]


def finish(coords, speeds, sums, out_x, out_v, out_e):
    out_x[...] = coords[...]
    out_v[...] = speeds[...]
    out_e[...] = sums[...]


def on_device(sizes, positions, velocities, send_list, pair_list, constraint_flags):
    clusters = positions.shape[2]
    slots = pair_list.shape[1]
    tiles = slots // LANES
    count = sizes[0] * sizes[1] * sizes[2]
    unroll = max(u for u in range(1, 15) if tiles % u == 0)
    vmem = pl.BlockSpec(memory_space=pltpu.VMEM)
    f32 = jnp.float32
    coords, speeds, sums = pl.pallas_call(
        functools.partial(kernel, sizes, unroll),
        out_shape=(
            jax.ShapeDtypeStruct(positions.shape, f32),
            jax.ShapeDtypeStruct(velocities.shape, f32),
            jax.ShapeDtypeStruct((2, ITERS), f32),
        ),
        in_specs=[pl.BlockSpec(memory_space=pl.ANY)] * 5,
        out_specs=(vmem, vmem, vmem),
        scratch_shapes=[
            pltpu.VMEM(send_list.shape, jnp.int32),
            pltpu.VMEM((2, LANES), jnp.int32),
            pltpu.VMEM(pair_list.shape, jnp.int32),
            pltpu.VMEM(constraint_flags.shape, jnp.int32),
            pltpu.SemaphoreType.DMA((5,)),
            pltpu.VMEM((2 * slots, 3 * clusters), jnp.bfloat16),
            pltpu.VMEM((2 * clusters, clusters), jnp.bfloat16),
            pltpu.VMEM((tiles, 8, 8, LANES), f32),
            pltpu.VMEM((3, 3, 8, LANES), f32),
            pltpu.VMEM((6, 8, LANES), jnp.int32),
            pltpu.VMEM((3, 8, LANES), f32),
            pltpu.VMEM((6, 3, LANES), f32),
            pltpu.VMEM((3, 8, LANES), f32),
            pltpu.VMEM((6, 3, LANES), f32),
            pltpu.VMEM((3, 8, LANES), f32),
            pltpu.VMEM((6, 3, LANES), f32),
            pltpu.VMEM((3, 8, LANES), f32),
            pltpu.VMEM((6, 3, LANES), f32),
            pltpu.VMEM((48, 2 * slots), f32),
            pltpu.VMEM((3, 8, LANES), f32),
            pltpu.VMEM((3, 8, LANES), f32),
            pltpu.VMEM((8, LANES), f32),
            pltpu.VMEM((2 * ITERS, 8, LANES), f32),
            pltpu.VMEM((8, LANES), f32),
            pltpu.VMEM((count, 8, LANES), f32),
            pltpu.SemaphoreType.DMA((7,)),
            pltpu.SemaphoreType.DMA((7,)),
            pltpu.SemaphoreType.DMA((7,)),
            pltpu.SemaphoreType.DMA((7,)),
            pltpu.SemaphoreType.DMA((count,)),
            pltpu.SemaphoreType.DMA((count,)),
        ],
        compiler_params=pltpu.CompilerParams(collective_id=0, has_side_effects=True),
    )(positions, velocities, send_list, pair_list, constraint_flags)
    results = (coords, speeds, sums)
    coords, speeds, sums = pl.pallas_call(
        finish,
        out_shape=tuple(jax.ShapeDtypeStruct(r.shape, f32) for r in results),
        in_specs=[vmem] * 3,
        out_specs=(vmem, vmem, vmem),
    )(*results)
    return coords, speeds, sums.T


def solution(mesh):
    sizes = tuple(mesh.shape[axis] for axis in AXES)
    split = ("runs", "gx", "gy", "gz")
    return jax.shard_map(
        functools.partial(on_device, sizes),
        mesh=mesh,
        in_specs=(
            P(None, None, split),
            P(None, None, split),
            P(split),
            P(None, split),
            P(None, split),
        ),
        out_specs=(P(None, None, split), P(None, None, split), P("runs", None)),
        check_vma=False,
    )
```
